32 devices in a mesh: lat: 8 (over y, x, core), lon: 4 (over z).
Axes of the slice: x: 2, y: 2, z: 4, core: 2. Of those that a mesh axis runs over, the one named last changes fastest.
Arguments:
- inputs: bfloat16 [128, 384, 256], P('lat', 'lon'), may hold values from -6 to 6
- first_filter: bfloat16 [3, 3, 256, 256], replicated, may hold values from -0.125 to 0.125
- second_filter: bfloat16 [3, 3, 256, 256], replicated, may hold values from -0.125 to 0.125
- cotangent: bfloat16 [128, 384, 256], P('lat', 'lon'), may hold values from -30 to 30
Outputs:
- input_grad: bfloat16 [128, 384, 256], P('lat', 'lon')
- first_grad: float32 [3, 3, 256, 256], replicated
- second_grad: float32 [3, 3, 256, 256], replicated
The draws below stay inside these ranges and needn't reach their ends.
All inputs are finite; a program needn't handle non-finite values.
Results may differ from the reference program's by a relative error of at most 0.0061.
Values may be sent and summed in bfloat16 or wider, within the bound.
No kernel may reach another device: no remote copies, remote signals or barrier semaphores. Data moves between devices by JAX's collectives and lax.ppermute only.
A program may use at most 64 MiB of HBM per device.

```python
import jax
import jax.numpy as jnp
from jax import lax

CH = 256
NLAT = 128
NLON = 384


def draw_cotangent(key, part):
    lat_pos = jnp.arange(NLAT, dtype=jnp.float32)[:, None, None] / NLAT
    lon_pos = jnp.arange(NLON, dtype=jnp.float32)[None, :, None] / NLON
    rough = jax.random.uniform(jax.random.fold_in(key, 7), (NLAT, NLON, 1), jnp.float32, 0.5, 1.5)
    base = jnp.clip(jax.random.normal(key, (NLAT, NLON, CH), jnp.float32), -6.0, 6.0)
    scale = jnp.exp(jnp.log(3.0) * (lat_pos + lon_pos))
    return jnp.clip(base * rough * scale / 3.0, -30.0, 30.0).astype(jnp.bfloat16)


def levels(stream_key, shape, pieces, low, top_value):
    def one(position, shards_of):
        steps = jax.random.uniform(jax.random.fold_in(jax.random.fold_in(stream_key, 6), position), (shards_of,), jnp.float32, low / len(pieces), top_value / len(pieces))
        return jnp.repeat(jnp.exp(steps), shape[position] // shards_of).reshape((-1,) + (1,) * (len(shape) - position - 1))

    level = one(*pieces[0])
    for cut in pieces[1:]:
        level = level * one(*cut)
    return level


def gaussian(stream_key, extent, deviation, reach, cuts=(), kind=jnp.bfloat16):
    result = jax.random.normal(stream_key, extent, jnp.float32) * deviation
    if len(cuts) > 0:
        result = levels(stream_key, extent, cuts, -0.22, 0.18) * result
    return jnp.clip(result, min=-reach, max=reach).astype(kind)


def setup_inputs(seed: int = 0) -> dict:
    keys = jax.random.split(jax.random.key(seed), 5)
    return {
        "inputs": gaussian(keys[0], (NLAT, NLON, CH), 1.0, 6.0, ((0, 8), (1, 4))),
        "first_filter": gaussian(keys[1], (3, 3, CH, CH), (9 * CH) ** -0.5, 0.125),
        "second_filter": gaussian(keys[2], (3, 3, CH, CH), (9 * CH) ** -0.5, 0.125),
        "cotangent": draw_cotangent(jax.random.fold_in(keys[4], 71), 0),
    }


def pad_field(field):
    wrapped = jnp.concatenate([field[:, -1:], field, field[:, :1]], axis=1)
    zeros = jnp.zeros((1,) + wrapped.shape[1:], wrapped.dtype)
    return jnp.concatenate([zeros, wrapped, zeros], axis=0)

def conv_taps(padded, weight, rows, cols, flipped):
    total = jnp.zeros((rows * cols, weight.shape[3] if not flipped else weight.shape[2]), jnp.float32)
    for first in range(3):
        for second in range(3):
            piece = padded[first:first + rows, second:second + cols, :].reshape(rows * cols, -1)
            if flipped:
                total = total + lax.dot_general(piece, weight[2 - first, 2 - second], (((1,), (1,)), ((), ())), preferred_element_type=jnp.float32)
            else:
                total = total + jnp.dot(piece, weight[first, second], preferred_element_type=jnp.float32)
    return total.reshape(rows, cols, -1)

def filter_grad(padded, delta, rows, cols):
    flat = delta.reshape(rows * cols, -1)
    taps = []
    for first in range(3):
        for second in range(3):
            piece = padded[first:first + rows, second:second + cols, :].reshape(rows * cols, -1)
            taps.append(lax.dot_general(piece, flat, (((0,), (0,)), ((), ())), preferred_element_type=jnp.float32))
    return jnp.stack(taps).reshape(3, 3, flat.shape[1], flat.shape[1])

def gelu_value(value):
    return value * 0.5 * (1.0 + jax.scipy.special.erf(value * 0.7071067811865476))

def gelu_slope(value):
    return 0.5 * (1.0 + jax.scipy.special.erf(value * 0.7071067811865476)) + value * jnp.exp(-0.5 * value * value) * 0.3989422804014327

def reference(inputs, first_filter, second_filter, cotangent):
    rows, cols = (inputs.shape[0], inputs.shape[1])
    padded_in = pad_field(inputs)
    hidden_one = conv_taps(padded_in, first_filter, rows, cols, False)
    act = gelu_value(hidden_one).astype(jnp.bfloat16)
    padded_act = pad_field(act)
    hidden_two = conv_taps(padded_act, second_filter, rows, cols, False)
    delta_two = (cotangent.astype(jnp.float32) * gelu_slope(hidden_two)).astype(jnp.bfloat16)
    second_grad = filter_grad(padded_act, delta_two, rows, cols)
    act_grad = conv_taps(pad_field(delta_two), second_filter, rows, cols, True)
    delta_one = (act_grad * gelu_slope(hidden_one)).astype(jnp.bfloat16)
    first_grad = filter_grad(padded_in, delta_one, rows, cols)
    input_grad = conv_taps(pad_field(delta_one), first_filter, rows, cols, True).astype(jnp.bfloat16)
    return (input_grad, first_grad, second_grad)
```

```python
import functools

import jax
import jax.numpy as jnp
from jax import lax
from jax.experimental import pallas as pl
from jax.experimental.pallas import tpu as pltpu
from jax.sharding import PartitionSpec as P

F32 = jnp.float32
BF16 = jnp.bfloat16
AXES = ("lat", "lon")
TAIL = 16
ROWS_PER_DOT = 2


def gelu_parts(h):
    cdf = 0.5 * (1.0 + lax.erf(h * 0.7071067811865476))
    slope = cdf + h * jnp.exp(-0.5 * h * h) * 0.3989422804014327
    return h * cdf, slope


def put(ref, row, pitch, value):
    at = pl.ds(row * pitch, pitch)
    ref[0, at, :] = pltpu.roll(value, 1, 0).astype(BF16)
    ref[1, at, :] = value.astype(BF16)
    ref[2, at, :] = pltpu.roll(value, pitch - 1, 0).astype(BF16)


def conv(source, weight, first, rows, pitch, flipped):
    total = None
    for a in range(3):
        for b in range(3):
            row = first + (2 - a if flipped else a)
            shift = 2 - b if flipped else b
            part = jnp.dot(
                source[shift, pl.ds(row * pitch, rows * pitch), :],
                weight[a, b],
                preferred_element_type=F32,
            )
            total = part if total is None else total + part
    return total


def filter_grad(source, first, delta, delta_first, rows, cols, pitch, out):
    flat = jnp.concatenate(
        [delta[1, pl.ds((delta_first + i) * pitch, cols), :] for i in range(rows)], axis=0
    ).T
    for a in range(3):
        for b in range(3):
            cells = jnp.concatenate(
                [source[b, pl.ds((first + a + i) * pitch, cols), :] for i in range(rows)], axis=0
            )
            part = jnp.dot(flat, cells, preferred_element_type=F32)
            out[a, b] = part.T.astype(out.dtype)


def spans(rows):
    return [(s, min(ROWS_PER_DOT, rows - s)) for s in range(0, rows, ROWS_PER_DOT)]


def kernel(
    R, C, edge, x, c, low, high, tail, w1, w2, w1t, w2t,
    input_grad, first_grad, second_grad, xs, acts, slopes, d2, d1,
):
    pitch = C + TAIL
    ch = x.shape[-1]
    for r in range(R + 8):
        own = low[r] if r < 4 else x[r - 4] if r < R + 4 else high[r - R - 4]
        put(xs, r, pitch, jnp.concatenate([own.astype(F32), tail[r].astype(F32)], axis=0))
    for s, n in spans(R + 6):
        h = conv(xs, w1, s, n, pitch, False)
        for k in range(n):
            value, slope = gelu_parts(h[k * pitch : (k + 1) * pitch])
            put(acts, s + k, pitch, value)
            slopes[pl.ds((s + k) * pitch, pitch), :] = slope
    for side, start in ((0, 0), (1, R + 3)):

        @pl.when(edge[side] == 1)
        def _():
            at = pl.ds(start * pitch, 3 * pitch)
            for b in range(3):
                acts[b, at, :] = jnp.zeros((3 * pitch, ch), BF16)
            slopes[at, :] = jnp.zeros((3 * pitch, ch), F32)

    for s, n in spans(R + 4):
        h = conv(acts, w2, s, n, pitch, False)
        for k in range(n):
            r = s + k
            own = low[r + 4] if r < 2 else c[r - 2] if r < R + 2 else high[r - R + 2]
            cot = jnp.concatenate([own.astype(F32), tail[R + 8 + r].astype(F32)], axis=0)
            put(d2, r, pitch, cot * gelu_parts(h[k * pitch : (k + 1) * pitch])[1])
    filter_grad(acts, 2, d2, 2, R, C, pitch, second_grad)
    for s, n in spans(R + 2):
        h = conv(d2, w2t, s, n, pitch, True)
        for k in range(n):
            at = pl.ds((s + k + 2) * pitch, pitch)
            put(d1, s + k, pitch, h[k * pitch : (k + 1) * pitch] * slopes[at, :])
    filter_grad(xs, 3, d1, 1, R, C, pitch, first_grad)
    for s, n in spans(R):
        h = conv(d1, w1t, s, n, pitch, True)
        for k in range(n):
            input_grad[s + k] = h[k * pitch : k * pitch + C].astype(BF16)


def block_step(edge, x, c, low, high, tail, w1, w2):
    R, C, ch = x.shape
    pitch = C + TAIL
    vmem = pl.BlockSpec(memory_space=pltpu.VMEM)
    filters = jax.ShapeDtypeStruct(w1.shape, BF16)
    return pl.pallas_call(
        functools.partial(kernel, R, C),
        out_shape=[jax.ShapeDtypeStruct(x.shape, BF16), filters, filters],
        in_specs=[pl.BlockSpec(memory_space=pltpu.SMEM)] + [vmem] * 9,
        out_specs=[vmem] * 3,
        scratch_shapes=[
            pltpu.VMEM((3, (R + 8) * pitch, ch), BF16),
            pltpu.VMEM((3, (R + 6) * pitch, ch), BF16),
            pltpu.VMEM(((R + 6) * pitch, ch), F32),
            pltpu.VMEM((3, (R + 4) * pitch, ch), BF16),
            pltpu.VMEM((3, (R + 2) * pitch, ch), BF16),
        ],
        compiler_params=pltpu.CompilerParams(vmem_limit_bytes=40 * 2**20),
    )(edge, x, c, low, high, tail, w1, w2, jnp.swapaxes(w1, 2, 3), jnp.swapaxes(w2, 2, 3))


def halos(x, c):
    R, C, ch = x.shape
    L, Z = lax.axis_size("lat"), lax.axis_size("lon")
    up = [(i, i + 1) for i in range(L - 1)]
    down = [(i + 1, i) for i in range(L - 1)]
    low = lax.ppermute(jnp.concatenate([x[R - 4 :], c[R - 2 :]], axis=0), "lat", up)
    high = lax.ppermute(jnp.concatenate([x[:4], c[:2]], axis=0), "lat", down)

    def columns(start):
        parts = [low[:4], x, high[:4], low[4:], c, high[4:]]
        taken = jnp.concatenate([p[:, start : start + 4] for p in parts], axis=0)
        return taken.reshape(-1, 8, ch)

    east = [(i, (i + 1) % Z) for i in range(Z)]
    west = [(d, s) for s, d in east]
    left = lax.ppermute(columns(C - 4), "lon", east).reshape(-1, 4, ch)
    right = lax.ppermute(columns(0), "lon", west).reshape(-1, 4, ch)
    gap = jnp.zeros((left.shape[0], TAIL - 8, ch), BF16)
    return low, high, jnp.concatenate([right, gap, left], axis=1)


def total(part):
    L, Z = lax.axis_size("lat"), lax.axis_size("lon")
    N = L * Z
    lat = [Z << k for k in range(L.bit_length() - 1)]
    lon = [1 << k for k in range(Z.bit_length() - 1)]
    core, rest = lat[0], lat[1:]
    steps = [(core, core)] + list(zip(rest + lon, rest[::-1] + lon))
    me = lax.axis_index("lat") * Z + lax.axis_index("lon")
    halved = steps[: len(steps) - min(2, len(lon))]

    def exchange(v, bits):
        pairs = [(i, i ^ bits[1 if i & core else 0]) for i in range(N)]
        return lax.ppermute(v, AXES, pairs)

    def side(bits):
        return (me // jnp.where(me & core == 0, bits[0], bits[1])) % 2

    v = part
    for bits in halved:
        half = v.shape[0] // 2
        give = lax.dynamic_slice_in_dim(v, (1 - side(bits)) * half, half).astype(BF16)
        keep = lax.dynamic_slice_in_dim(v, side(bits) * half, half).astype(F32)
        v = keep + exchange(give, bits).astype(F32)
    for bits in steps[len(halved) :]:
        v = v.astype(BF16)
        v = v.astype(F32) + exchange(v, bits).astype(F32)
    v = v.astype(BF16)
    for bits in halved[::-1]:
        other = exchange(v, bits)
        v = jnp.where(
            side(bits) == 0, jnp.concatenate([v, other]), jnp.concatenate([other, v])
        )
    return v.astype(F32)


def body(inputs, first_filter, second_filter, cotangent):
    index, count = lax.axis_index("lat"), lax.axis_size("lat")
    edge = jnp.stack([index == 0, index == count - 1]).astype(jnp.int32)
    low, high, tail = halos(inputs, cotangent)
    input_grad, first_part, second_part = block_step(
        edge, inputs, cotangent, low, high, tail, first_filter, second_filter
    )
    ch = inputs.shape[-1]
    second_grad = total(second_part.reshape(-1, ch)).reshape(second_filter.shape)
    first_grad = total(first_part.reshape(-1, ch)).reshape(first_filter.shape)
    return input_grad, first_grad, second_grad


def solution(mesh):
    in_specs = (P("lat", "lon", None), P(), P(), P("lat", "lon", None))
    out_specs = (P("lat", "lon", None), P(), P())
    return jax.shard_map(body, mesh=mesh, in_specs=in_specs, out_specs=out_specs, check_vma=False)
```

```python
import functools

import jax
import jax.numpy as jnp
from jax import lax
from jax.experimental import pallas as pl
from jax.experimental.pallas import tpu as pltpu
from jax.sharding import PartitionSpec as P


F32 = jnp.float32
BF16 = jnp.bfloat16
AXES = ("lat", "lon")
TAIL = 16
ROWS_PER_DOT = 2
FULL = (2, 2)

HBM = pl.BlockSpec(memory_space=pltpu.HBM)
VMEM = pl.BlockSpec(memory_space=pltpu.VMEM)
SMEM = pl.BlockSpec(memory_space=pltpu.SMEM)


def call(body, outs, in_specs, scratch, limit, flops=0, out_specs=None, aliases=None):
    cost = pl.CostEstimate(flops=flops, bytes_accessed=0, transcendentals=0) if flops else None
    run = pl.pallas_call(
        body,
        out_shape=outs,
        in_specs=in_specs,
        out_specs=out_specs or [VMEM] * len(outs),
        scratch_shapes=scratch,
        cost_estimate=cost,
        input_output_aliases=aliases or {},
        compiler_params=pltpu.CompilerParams(vmem_limit_bytes=limit * 2**20),
    )

    def placed(*args):
        return run(
            *(
                pltpu.with_memory_space_constraint(a, pltpu.HBM) if spec is HBM else a
                for a, spec in zip(args, in_specs)
            )
        )

    return placed


def gelu_parts(h):
    cdf = 0.5 * (1.0 + lax.erf(h * 0.7071067811865476))
    slope = cdf + h * jnp.exp(-0.5 * h * h) * 0.3989422804014327
    return h * cdf, slope


def put(ref, row, pitch, value):
    at = pl.ds(row * pitch, pitch)
    ref[0, at, :] = pltpu.roll(value, 1, 0).astype(BF16)
    ref[1, at, :] = value.astype(BF16)
    ref[2, at, :] = pltpu.roll(value, pitch - 1, 0).astype(BF16)


def extended_row(own, index, left, right):
    a, b = right[index // 2].astype(F32), left[index // 2].astype(F32)
    if index % 2:
        a = pltpu.roll(a, 4, 0)
    else:
        b = pltpu.roll(b, 4, 0)
    return jnp.concatenate([own.astype(F32), a, b], axis=0)


def conv(source, weight, first, rows, pitch, flipped):
    total = None
    for a in range(3):
        for b in range(3):
            row = first + (2 - a if flipped else a)
            shift = 2 - b if flipped else b
            part = jnp.dot(
                source[shift, pl.ds(row * pitch, rows * pitch), :],
                weight[a, b],
                preferred_element_type=F32,
            )
            total = part if total is None else total + part
    return total


def filter_grad(source, first, delta_rows, R, C, pitch, core, halves, keep, give):
    flat = jnp.concatenate(delta_rows, axis=0).T
    for a in range(3):
        for b in range(3):
            cells = jnp.concatenate(
                [source[b, pl.ds((first + a + i) * pitch, C), :] for i in range(R)], axis=0
            )
            part = jnp.dot(flat, cells, preferred_element_type=F32).T
            n = part.shape[0] // 2
            for k in range(2):
                piece = 2 * (3 * a + b) + k
                slot = core if piece < 9 else 1 - core
                halves[slot, pl.ds(piece % 9 * n, n), :] = part[k * n : (k + 1) * n]
    keep[...] = halves[0]
    give[...] = halves[1].astype(BF16)


def spans(rows):
    return [(s, min(ROWS_PER_DOT, rows - s)) for s in range(0, rows, ROWS_PER_DOT)]


def transpose_filters(w1, w2, w1t, w2t):
    for source, out in ((w1, w1t), (w2, w2t)):
        for a in range(3):
            for b in range(3):
                out[a, b] = source[a, b].T


def widen(rows, mine, info, part, *refs):
    out, staged, sems = refs[-3:]
    base = rows * (info[2] if mine else 1 - info[2])
    chunk = rows // 2
    copies = []
    for i in range(2):
        staged[i] = part[pl.ds(i * chunk, chunk), :].astype(F32)
        to = out.at[pl.ds(base + i * chunk, chunk)]
        copies.append(pltpu.make_async_copy(staged.at[i], to, sems.at[i]))
        copies[i].start()
    for copy in copies:
        copy.wait()


def pack_rows(R, x, c, up, down, sems):
    moves = [
        (x.at[pl.ds(R - 4, 4)], up.at[pl.ds(0, 4)]),
        (c.at[pl.ds(R - 2, 2)], up.at[pl.ds(4, 2)]),
        (x.at[pl.ds(0, 4)], down.at[pl.ds(0, 4)]),
        (c.at[pl.ds(0, 2)], down.at[pl.ds(4, 2)]),
    ]
    copies = [pltpu.make_async_copy(s, d, sems.at[i]) for i, (s, d) in enumerate(moves)]
    for copy in copies:
        copy.start()
    for copy in copies:
        copy.wait()


def pair_columns(east, west, block, first, second):
    upper = lax.broadcasted_iota(jnp.int32, first[0].shape, 0) < 4
    (ha, ta), (hb, tb) = first, second
    west[block] = jnp.where(upper, ha, pltpu.roll(hb, 4, 0)).astype(BF16)
    east[block] = jnp.where(upper, pltpu.roll(ta, 4, 0), tb).astype(BF16)


def ends(ref, row, C):
    return ref[row, 0:8, :].astype(F32), ref[row, C - 8 : C, :].astype(F32)


def own_columns(R, C, x, c, east, west, xh, xt, ch, ct, sems):
    moves = [(x, 0, xh), (x, C - 8, xt), (c, 0, ch), (c, C - 8, ct)]
    copies = [
        pltpu.make_async_copy(s.at[:, pl.ds(at, 8), :], d, sems.at[i])
        for i, (s, at, d) in enumerate(moves)
    ]
    for copy in copies:
        copy.start()
    for copy in copies:
        copy.wait()
    for k, (heads, tails) in enumerate(((xh, xt), (ch, ct))):
        for r in range(0, R, 2):
            rows = [(heads[i].astype(F32), tails[i].astype(F32)) for i in (r, r + 1)]
            pair_columns(east, west, k * R // 2 + r // 2, *rows)


def all_columns(R, C, own_east, own_west, low, high, east, west):
    n = R // 2
    for own, out in ((own_east, east), (own_west, west)):
        out[2 : 2 + n] = own[0:n]
        out[5 + n : 5 + 2 * n] = own[n : 2 * n]
    for ref, row, block in (
        (low, 0, 0), (low, 2, 1), (high, 0, 2 + n), (high, 2, 3 + n),
        (low, 4, 4 + n), (high, 4, 5 + 2 * n),
    ):
        pair_columns(east, west, block, ends(ref, row, C), ends(ref, row + 1, C))


def forward_kernel(
    R, C, info, x_hbm, c_hbm, w1_hbm, w2_hbm, low, high, left, right,
    d2_hbm, slopes_hbm, keep, give, x, c, w1, w2, xs, acts, halves, d2, slopes, sems,
):
    pitch = C + TAIL
    channels = x.shape[-1]
    copies = [
        pltpu.make_async_copy(s, d, sems.at[i])
        for i, (s, d) in enumerate(((x_hbm, x), (w1_hbm, w1), (c_hbm, c), (w2_hbm, w2)))
    ]
    for copy in copies:
        copy.start()
    copies[0].wait()
    for r in range(R + 8):
        own = low[r] if r < 4 else x[r - 4] if r < R + 4 else high[r - R - 4]
        put(xs, r, pitch, extended_row(own, r, left, right))
    copies[1].wait()
    for s, n in spans(R + 6):
        h = conv(xs, w1, s, n, pitch, False)
        for k in range(n):
            r = s + k
            value, slope = gelu_parts(h[k * pitch : (k + 1) * pitch])
            put(acts, r, pitch, value)
            if 2 <= r < R + 4:
                slopes[pl.ds((r - 2) * pitch, pitch), :] = slope
    for side, start, row in ((0, 0, 0), (1, R + 3, R + 1)):

        @pl.when(info[side] == 1)
        def _():
            at = pl.ds(start * pitch, 3 * pitch)
            for b in range(3):
                acts[b, at, :] = jnp.zeros((3 * pitch, channels), BF16)
            slopes[pl.ds(row * pitch, pitch), :] = jnp.zeros((pitch, channels), F32)

    slopes_out = pltpu.make_async_copy(slopes, slopes_hbm, sems.at[4])
    slopes_out.start()
    copies[2].wait()
    copies[3].wait()
    for s, n in spans(R + 4):
        h = conv(acts, w2, s, n, pitch, False)
        for k in range(n):
            r = s + k
            own = low[r + 4] if r < 2 else c[r - 2] if r < R + 2 else high[r - R + 2]
            cot = extended_row(own, R + 8 + r, left, right)
            slope = gelu_parts(h[k * pitch : (k + 1) * pitch])[1]
            d2[pl.ds(r * pitch, pitch), :] = (cot * slope).astype(BF16)
    d2_out = pltpu.make_async_copy(d2, d2_hbm, sems.at[5])
    d2_out.start()
    rows = [d2[pl.ds((2 + i) * pitch, C), :] for i in range(R)]
    filter_grad(acts, 2, rows, R, C, pitch, info[2], halves, keep, give)
    slopes_out.wait()
    d2_out.wait()


def backward_kernel(
    R, C, info, x_hbm, d2_hbm, slopes_hbm, w2t_hbm, low, high, left, right,
    d1_hbm, keep, give, x, d2, slopes, w2t, d1, xs, d2s, halves, sems,
):
    pitch = C + TAIL
    moves = ((d2_hbm, d2), (w2t_hbm, w2t), (slopes_hbm, slopes), (x_hbm, x))
    copies = [pltpu.make_async_copy(s, d, sems.at[i]) for i, (s, d) in enumerate(moves)]
    for copy in copies:
        copy.start()
    copies[0].wait()
    for r in range(R + 4):
        put(d2s, r, pitch, d2[pl.ds(r * pitch, pitch), :].astype(F32))
    for copy in copies[1:]:
        copy.wait()
    for s, n in spans(R + 2):
        h = conv(d2s, w2t, s, n, pitch, True)
        for k in range(n):
            r = s + k
            at = pl.ds(r * pitch, pitch)
            d1[at, :] = (h[k * pitch : (k + 1) * pitch] * slopes[at, :]).astype(BF16)
            own = low[3] if r == 0 else x[r - 1] if r <= R else high[0]
            put(xs, r, pitch, extended_row(own, r + 3, left, right))
    d1_out = pltpu.make_async_copy(d1, d1_hbm, sems.at[4])
    d1_out.start()
    rows = [d1[pl.ds((1 + i) * pitch, C), :] for i in range(R)]
    filter_grad(xs, 0, rows, R, C, pitch, info[2], halves, keep, give)
    d1_out.wait()


def input_kernel(R, C, d1_hbm, w1t_hbm, input_grad, d1, w1t, d1s, sems):
    pitch = C + TAIL
    moves = ((d1_hbm, d1), (w1t_hbm, w1t))
    copies = [pltpu.make_async_copy(s, d, sems.at[i]) for i, (s, d) in enumerate(moves)]
    for copy in copies:
        copy.start()
    copies[0].wait()
    for r in range(R + 2):
        put(d1s, r, pitch, d1[pl.ds(r * pitch, pitch), :].astype(F32))
    copies[1].wait()
    for s, n in spans(R):
        h = conv(d1s, w1t, s, n, pitch, True)
        for k in range(n):
            input_grad[s + k] = h[k * pitch : k * pitch + C].astype(BF16)


def halos(x, c):
    R, C, ch = x.shape
    L, Z = lax.axis_size("lat"), lax.axis_size("lon")
    sems = pltpu.SemaphoreType.DMA((4,))
    rows = pltpu.VMEM((6, C, ch), BF16)
    up, down = call(functools.partial(pack_rows, R), [rows] * 2, [HBM] * 2, [sems], 8)(x, c)
    low = lax.ppermute(up, "lat", [(i, i + 1) for i in range(L - 1)])
    high = lax.ppermute(down, "lat", [(i + 1, i) for i in range(L - 1)])
    own = pltpu.VMEM((R, 8, ch), BF16)
    own_east, own_west = call(
        functools.partial(own_columns, R, C),
        [own] * 2,
        [HBM] * 2,
        [pltpu.VMEM((R, 8, ch), BF16)] * 4 + [sems],
        8,
    )(x, c)
    every = pltpu.VMEM((R + 6, 8, ch), BF16)
    east, west = call(functools.partial(all_columns, R, C), [every] * 2, [VMEM] * 4, [], 8)(
        own_east, own_west, low, high
    )
    ring = [(i, (i + 1) % Z) for i in range(Z)]
    left = lax.ppermute(east, "lon", ring)
    right = lax.ppermute(west, "lon", [(d, s) for s, d in ring])
    return low, high, left, right


def total(keep, give, info, full):
    L, Z = lax.axis_size("lat"), lax.axis_size("lon")
    N = L * Z
    lat = [Z << k for k in range(L.bit_length() - 1)]
    lon = [1 << k for k in range(Z.bit_length() - 1)]
    core, rest = lat[0], lat[1:]
    steps = list(zip(rest + lon, rest[::-1] + lon))
    me = lax.axis_index("lat") * Z + lax.axis_index("lon")
    halved = steps[: len(steps) - min(full, len(lon))]

    def exchange(v, bits):
        pairs = [(i, i ^ bits[1 if i & core else 0]) for i in range(N)]
        return lax.ppermute(v, AXES, pairs)

    def side(bits):
        return (me // jnp.where(me & core == 0, bits[0], bits[1])) % 2

    v = keep + exchange(give, (core, core)).astype(F32)
    for bits in halved:
        half = v.shape[0] // 2
        sent = lax.dynamic_slice_in_dim(v, (1 - side(bits)) * half, half).astype(BF16)
        kept = lax.dynamic_slice_in_dim(v, side(bits) * half, half)
        v = kept + exchange(sent, bits).astype(F32)
    for bits in steps[len(halved) :]:
        v = v.astype(BF16)
        v = v.astype(F32) + exchange(v, bits).astype(F32)
    v = v.astype(BF16)
    for bits in halved[::-1]:
        other = exchange(v, bits)
        v = jnp.where(
            side(bits) == 0, jnp.concatenate([v, other]), jnp.concatenate([other, v])
        )
    rows, ch = v.shape
    other = exchange(v, (core, core))
    whole = [pltpu.HBM((2 * rows, ch), F32)]
    scratch = [pltpu.VMEM((2, rows // 2, ch), F32), pltpu.SemaphoreType.DMA((2,))]
    own = functools.partial(widen, rows, True)
    (out,) = call(own, whole, [SMEM, VMEM], scratch, 8, out_specs=[HBM])(info, v)
    rest = functools.partial(widen, rows, False)
    (out,) = call(
        rest, whole, [SMEM, VMEM, HBM], scratch, 8, out_specs=[HBM], aliases={2: 0}
    )(info, other, out)
    return out


def body(inputs, first_filter, second_filter, cotangent):
    R, C, ch = inputs.shape
    pitch = C + TAIL
    index, count = lax.axis_index("lat"), lax.axis_size("lat")
    info = jnp.stack([index == 0, index == count - 1, index % 2 == 1]).astype(jnp.int32)
    low, high, left, right = halos(inputs, cotangent)

    def space(*dims, dtype=BF16):
        return pltpu.VMEM(dims, dtype)

    flipped = pltpu.HBM(first_filter.shape, BF16)
    w1t, w2t = call(transpose_filters, [flipped] * 2, [VMEM] * 2, [], 12)(
        first_filter, second_filter
    )
    half = 9 * ch // 2
    halves = space(2, half, ch, dtype=F32)
    parts = [space(half, ch, dtype=F32), space(half, ch)]
    per_cell = 18 * ch * ch
    cells2, cells1 = (R + 4) * pitch, (R + 2) * pitch
    d2, slopes, keep, give = call(
        functools.partial(forward_kernel, R, C),
        [pltpu.HBM((cells2, ch), BF16), pltpu.HBM((cells1, ch), F32)] + parts,
        [SMEM] + [HBM] * 4 + [VMEM] * 4,
        [space(R, C, ch)] * 2 + [space(*first_filter.shape)] * 2
        + [space(3, (R + 8) * pitch, ch), space(3, (R + 6) * pitch, ch), halves]
        + [space(cells2, ch), space(cells1, ch, dtype=F32), pltpu.SemaphoreType.DMA((6,))],
        32,
        per_cell * ((2 * R + 10) * pitch + R * C),
        [HBM] * 2 + [VMEM] * 2,
    )(info, inputs, cotangent, first_filter, second_filter, low, high, left, right)
    second_grad = total(keep, give, info, FULL[0])
    backward = call(
        functools.partial(backward_kernel, R, C),
        [pltpu.HBM((cells1, ch), BF16)] + parts,
        [SMEM] + [HBM] * 4 + [VMEM] * 4,
        [space(R, C, ch), space(cells2, ch), space(cells1, ch, dtype=F32)]
        + [space(*second_filter.shape), space(cells1, ch)]
        + [space(3, cells1, ch), space(3, cells2, ch), halves, pltpu.SemaphoreType.DMA((5,))],
        32,
        per_cell * (cells1 + R * C),
        [HBM] + [VMEM] * 2,
    )
    d1, keep, give = backward(info, inputs, d2, slopes, w2t, low, high, left, right)
    first_grad = total(keep, give, info, FULL[1])
    last = call(
        functools.partial(input_kernel, R, C),
        [jax.ShapeDtypeStruct((R, C, ch), BF16)],
        [HBM] * 2,
        [space(cells1, ch), space(*first_filter.shape), space(3, cells1, ch)]
        + [pltpu.SemaphoreType.DMA((2,))],
        16,
        per_cell * R * pitch,
    )
    (input_grad,) = last(d1, w1t)
    return (
        input_grad,
        first_grad.reshape(first_filter.shape),
        second_grad.reshape(second_filter.shape),
    )


def solution(mesh):
    in_specs = (P("lat", "lon", None), P(), P(), P("lat", "lon", None))
    out_specs = (P("lat", "lon", None), P(), P())
    return jax.shard_map(
        body,
        mesh=mesh,
        in_specs=in_specs,
        out_specs=out_specs,
        check_vma=False,
    )
```
